32 devices in a mesh: wave: 16 (over z, y, core), lev: 2 (over x).
Axes of the slice: x: 2, y: 2, z: 4, core: 2. Of those that a mesh axis runs over, the one named last changes fastest.
Arguments:
- control: bfloat16 [2, 256, 256, 2, 512], P(None, 'wave', 'lev'), may hold values from -6 to 6
- wave_of_slot: int32 [256], replicated, may hold values from 0 to 255, each once
- legendre: bfloat16 [256, 256, 256], P('wave', 'lev'), may hold values from -0.375 to 0.375
- vertical: bfloat16 [4, 4, 128, 128], replicated, may hold values from -0.5 to 0.5
- points: int32 [256], P('wave'), may hold values from 128 to 512
- lat_band: int32 [256], P('wave'), may hold values from 0 to 7, never falling along the last dimension, each value on 1 to 64 neighbouring positions
- grid_scale: float32 [8, 512], P(None, 'lev'), may hold values from 0.5 to 2
- obs_weight: bfloat16 [256, 512, 512], P('wave', 'lev'), may hold values from 0.19921875 to 1
Outputs:
- increment: bfloat16 [2, 256, 512, 512], P(None, 'wave', 'lev')
- gradient: bfloat16 [2, 256, 256, 2, 512], P(None, 'wave', 'lev')
The draws below stay inside these ranges and needn't reach their ends.
Inputs may be any that keep to these rules, and one draw needn't show every extreme that they name: `wave_of_slot`: each zonal wavenumber 0 to 255 stands in exactly one slot. `lat_band`: band numbers never fall from one latitude to the next, and each band covers 1 to 64 latitudes.
All inputs are finite; a program needn't handle non-finite values.
Results may differ from the reference program's by a relative error of at most 0.007.
Values may be sent and summed in bfloat16 or wider, within the bound.
A program may use at most 192 MiB of HBM per device.

```python
import math
import jax
import jax.numpy as jnp
import numpy as np

WAVES = 256
LATITUDES = 256
LONGITUDES = 512
LEVELS = 128
VARIABLES = 4
COV_BANDS = 4
LAT_BANDS = 8
MEMBERS = 2
COLUMNS = 512


def plant(drawn, own_key, least, top_value):
    index_at = [jax.random.randint(jax.random.fold_in(own_key, axis), (), 0, length) for axis, length in enumerate(drawn.shape)]
    widest = drawn.shape.index(max(drawn.shape))
    next_to = index_at[:widest] + [(index_at[widest] + 1) % drawn.shape[widest]] + index_at[widest + 1:]
    return drawn.at[tuple(index_at)].set(least).at[tuple(next_to)].set(top_value)


def level_of(stream_key, extent, shards, least, high):
    gain, own = 1.0, jax.random.fold_in(stream_key, 6)
    for position, blocks in shards:
        steps = jnp.exp(jax.random.uniform(jax.random.fold_in(own, position), (blocks,), jnp.float32, least / len(shards), high / len(shards)))
        gain = gain * jnp.repeat(steps, extent[position] // blocks).reshape([-1 if axis == position else 1 for axis in range(len(extent))])
    return gain


def length_profile(count, total, most, skew):
    portions = [(1 << 20) // math.isqrt(rank ** skew) + 1 for rank in range(2, count + 1)]
    rest, holding = total - most - (count - 1), [1] * (count - 1)
    while rest > 0:
        candidates = [i for i in range(count - 1) if holding[i] < most]
        whole, remaining = sum([portions[i] for i in candidates]), rest
        for i in candidates:
            more = min(most - holding[i], max(1, remaining * portions[i] // whole), rest)
            holding[i] = holding[i] + more
            rest = rest - more
    return np.array([most] + holding)


def ragged_sizes(rng, count, total, reach, slope):
    if count == 2:
        one = jax.random.randint(rng, (), max(1, total - reach), min(reach, total - 1) + 1)
        return jnp.stack([one, total - one])
    tallies = jnp.asarray(length_profile(count, total, reach, slope), jnp.int32)
    couples = (count - 1) // 2
    donor, receiver = tallies[1:1 + 2 * couples:2], tallies[2:2 + 2 * couples:2]
    slack = jnp.minimum(donor - 1, reach - receiver)
    passed = jax.random.randint(jax.random.fold_in(rng, 1), (couples,), 0, 1 << 20) % (slack + 1)
    tallies = tallies.at[1:1 + 2 * couples:2].set(donor - passed).at[2:2 + 2 * couples:2].set(receiver + passed)
    return tallies[jax.random.permutation(jax.random.fold_in(rng, 2), count)]


def scatter_about(key, dims, spread, most, pieces=(), held_as=jnp.bfloat16):
    drawn = jax.random.normal(key, dims, jnp.float32) * spread
    if len(pieces) > 0:
        drawn = level_of(key, dims, pieces, -0.22, 0.18) * drawn
    return jnp.clip(drawn, min=-most, max=most).astype(held_as)


def setup_inputs(seed: int = 0) -> dict:
    splits = jax.random.split(jax.random.key(seed), 9)
    return {
        "control": scatter_about(splits[0], (MEMBERS, WAVES, WAVES, 2, COLUMNS), 1.0, 6.0, ((1, 16), (2, 2))),
        "wave_of_slot": jax.random.permutation(splits[1], WAVES).astype(jnp.int32),
        "legendre": scatter_about(splits[2], (WAVES, WAVES, LATITUDES), WAVES ** -0.5, 0.375, ((0, 16), (1, 2))),
        "vertical": scatter_about(splits[3], (COV_BANDS, VARIABLES, LEVELS, LEVELS), LEVELS ** -0.5, 0.5),
        "points": plant(jax.random.randint(splits[4], (LATITUDES,), LONGITUDES // 4, LONGITUDES + 1), jax.random.fold_in(splits[4], 1), LONGITUDES // 4, LONGITUDES).astype(jnp.int32),
        "lat_band": jnp.searchsorted(jnp.cumsum(ragged_sizes(splits[5], LAT_BANDS, LATITUDES, 2 * LATITUDES // LAT_BANDS, 1)), jnp.arange(LATITUDES), side="right").astype(jnp.int32),
        "grid_scale": jnp.clip(jnp.exp(math.log(2.0) - 1.3862944 * jax.random.uniform(splits[6], (LAT_BANDS, COLUMNS), jnp.float32) ** level_of(splits[6], (LAT_BANDS, COLUMNS), ((1, 2),), -0.2, 0.2)), 0.5, 2.0),
        "obs_weight": jnp.clip(jnp.exp(math.log(1.0) - 1.6133518 * jax.random.uniform(splits[7], (LATITUDES, COLUMNS, LONGITUDES), jnp.float32) ** level_of(splits[7], (LATITUDES, COLUMNS, LONGITUDES), ((0, 16), (1, 2)), -0.2, 0.2)), 0.19921875, 1.0).astype(jnp.bfloat16),
    }


def fourier_table(wave_ids, lat_points):
    lon_index = jnp.arange(LONGITUDES, dtype=jnp.int32)
    remainder = wave_ids[None, :, None] * lon_index[None, None, :] % lat_points[:, None, None]
    angles = 2.0 * math.pi * remainder.astype(jnp.float32) / lat_points.astype(jnp.float32)[:, None, None]
    factor = jnp.where(wave_ids == 0, 1.0, 2.0).astype(jnp.float32) / math.sqrt(4.0 * WAVES)
    inside = lon_index[None, None, :] < lat_points[:, None, None]
    cosine = jnp.where(inside, factor[None, :, None] * jnp.cos(angles), 0.0)
    sine = jnp.where(inside, -factor[None, :, None] * jnp.sin(angles), 0.0)
    return jnp.stack([cosine, sine], axis=2).astype(jnp.bfloat16)

def vertical_apply(field, vertical, live_rows, band_of, forward):
    shaped = field.astype(jnp.float32).reshape(WAVES, WAVES, 2, VARIABLES, LEVELS)
    matrices = vertical.astype(jnp.float32)
    form = 'skpam,alm->skpal' if forward else 'skpal,alm->skpam'
    summed = jnp.zeros(shaped.shape, jnp.float32)
    for index_band in range(COV_BANDS):
        partial_value = jnp.einsum(form, shaped, matrices[index_band])
        chosen = live_rows & (band_of == index_band)
        summed = summed + jnp.where(chosen[:, :, None, None, None], partial_value, 0.0)
    return summed.reshape(WAVES, WAVES, 2, COLUMNS).astype(jnp.bfloat16)

def reference(control, wave_of_slot, legendre, vertical, points, lat_band, grid_scale, obs_weight):
    row_index = jnp.arange(WAVES, dtype=jnp.int32)
    totals_n = wave_of_slot[:, None] + row_index[None, :]
    live_rows = totals_n <= WAVES - 1
    band_of = jnp.minimum(totals_n * COV_BANDS // WAVES, COV_BANDS - 1)
    fourier = fourier_table(wave_of_slot, points).astype(jnp.float32)
    table32 = legendre.astype(jnp.float32)
    lat_scale = grid_scale[lat_band]
    weight32 = obs_weight.astype(jnp.float32)
    increments = []
    gradients = []
    for member in range(MEMBERS):
        spectral = vertical_apply(control[member], vertical, live_rows, band_of, True)
        flat = spectral.astype(jnp.float32).reshape(WAVES, WAVES, 2 * COLUMNS)
        coeffs = jnp.einsum('skt,skq->stq', table32, flat).astype(jnp.bfloat16)
        coeffs32 = coeffs.astype(jnp.float32).reshape(WAVES, LATITUDES, 2, COLUMNS)
        synthesis = jnp.einsum('tspj,stpc->tcj', fourier, coeffs32)
        increment = (synthesis * lat_scale[:, :, None]).astype(jnp.bfloat16)
        weighted = (increment.astype(jnp.float32) * weight32 * lat_scale[:, :, None]).astype(jnp.bfloat16)
        adjoint_fourier = jnp.einsum('tspj,tcj->tspc', fourier, weighted.astype(jnp.float32)).astype(jnp.bfloat16)
        adjoint_flat = adjoint_fourier.astype(jnp.float32).reshape(LATITUDES, WAVES, 2 * COLUMNS)
        adjoint_coeffs = jnp.einsum('skt,tsq->skq', table32, adjoint_flat).astype(jnp.bfloat16)
        adjoint_coeffs = adjoint_coeffs.reshape(WAVES, WAVES, 2, COLUMNS)
        gradient = vertical_apply(adjoint_coeffs, vertical, live_rows, band_of, False)
        increments.append(increment)
        gradients.append(gradient)
    return (jnp.stack(increments, axis=0), jnp.stack(gradients, axis=0))
```

```python
import functools
import math

import jax
import jax.numpy as jnp
from jax import lax
from jax.experimental import pallas as pl
from jax.experimental.pallas import tpu as pltpu
from jax.sharding import PartitionSpec as P

WAVES = 256
LONGITUDES = 512
LEVELS = 128
VARIABLES = 4
COV_BANDS = 4


def fourier_table(wave_ids, lat_points):
    lon_index = jnp.arange(LONGITUDES, dtype=jnp.int32)
    remainder = wave_ids[None, :, None] * lon_index[None, None, :] % lat_points[:, None, None]
    angles = (
        2.0
        * math.pi
        * remainder.astype(jnp.float32)
        / lat_points.astype(jnp.float32)[:, None, None]
    )
    factor = jnp.where(wave_ids == 0, 1.0, 2.0).astype(jnp.float32) / math.sqrt(4.0 * WAVES)
    inside = lon_index[None, None, :] < lat_points[:, None, None]
    cosine = jnp.where(inside, factor[None, :, None] * jnp.cos(angles), 0.0)
    sine = jnp.where(inside, -factor[None, :, None] * jnp.sin(angles), 0.0)
    return jnp.stack([cosine, sine], axis=2).astype(jnp.bfloat16)


def vertical_apply(field, vertical, live_rows, band_of, forward):
    members, slots, rows_dev = (field.shape[0], field.shape[1], field.shape[2])
    shaped = field.reshape(members, slots, rows_dev, 2, VARIABLES, LEVELS)
    form = "eskpam,alm->eskpal" if forward else "eskpal,alm->eskpam"
    summed = jnp.zeros(shaped.shape, jnp.float32)
    for index_band in range(COV_BANDS):
        partial_value = jnp.einsum(
            form, shaped, vertical[index_band], preferred_element_type=jnp.float32
        )
        chosen = live_rows & (band_of == index_band)
        summed = summed + jnp.where(chosen[None, :, :, None, None, None], partial_value, 0.0)
    return summed.reshape(field.shape).astype(jnp.bfloat16)


def to_bands(values):
    return lax.all_to_all(values, "wave", split_axis=2, concat_axis=1, tiled=True)


def shards_plain(control, wave_of_slot, legendre, vertical, points, lat_band, grid_scale, obs_weight):
    members, slots, rows_dev = (control.shape[0], control.shape[1], control.shape[2])
    slot_start = lax.axis_index("wave") * slots
    row_start = lax.axis_index("lev") * rows_dev
    own_waves = lax.dynamic_slice_in_dim(wave_of_slot, slot_start, slots)
    row_index = row_start + jnp.arange(rows_dev, dtype=jnp.int32)
    totals_n = own_waves[:, None] + row_index[None, :]
    live_rows = totals_n <= WAVES - 1
    band_of = jnp.minimum(totals_n * COV_BANDS // WAVES, COV_BANDS - 1)
    spectral = vertical_apply(control, vertical, live_rows, band_of, True)
    columns = lax.all_to_all(spectral, "lev", split_axis=4, concat_axis=2, tiled=True)
    col_dev = columns.shape[4]
    width = 2 * col_dev
    all_rows = columns.shape[2]
    columns = columns.reshape(members, slots, all_rows, width)
    coeffs = jnp.einsum(
        "skt,eskq->estq",
        lax.all_gather(legendre, "lev", axis=1, tiled=True),
        columns,
        preferred_element_type=jnp.float32,
    )
    coeffs = coeffs.astype(jnp.bfloat16)
    by_lat = to_bands(coeffs)
    wave_count = by_lat.shape[1]
    lat_dev = by_lat.shape[2]
    by_lat = by_lat.reshape(members, wave_count, lat_dev, 2, col_dev)
    fourier = fourier_table(wave_of_slot, points)
    synthesis = jnp.einsum("tspj,estpc->etcj", fourier, by_lat, preferred_element_type=jnp.float32)
    chooser = (
        lat_band[:, None] == jnp.arange(grid_scale.shape[0], dtype=jnp.int32)[None, :]
    ).astype(jnp.float32)
    lat_scale = jnp.dot(chooser, grid_scale, precision=lax.Precision.HIGHEST)
    increment = (synthesis * lat_scale[None, :, :, None]).astype(jnp.bfloat16)
    weighted = (
        increment.astype(jnp.float32) * obs_weight.astype(jnp.float32) * lat_scale[None, :, :, None]
    ).astype(jnp.bfloat16)
    adjoint_fourier = jnp.einsum(
        "tspj,etcj->etspc", fourier, weighted, preferred_element_type=jnp.float32
    )
    adjoint_fourier = adjoint_fourier.astype(jnp.bfloat16).reshape(
        members, lat_dev, wave_count, width
    )
    band_rows = to_bands(adjoint_fourier)
    adjoint_coeffs = jnp.einsum(
        "skt,etsq->eskq",
        lax.all_gather(legendre, "lev", axis=1, tiled=True),
        band_rows,
        preferred_element_type=jnp.float32,
    )
    adjoint_coeffs = adjoint_coeffs.astype(jnp.bfloat16).reshape(
        members, slots, all_rows, 2, col_dev
    )
    rows_back = lax.all_to_all(adjoint_coeffs, "lev", split_axis=2, concat_axis=4, tiled=True)
    gradient = vertical_apply(rows_back, vertical, live_rows, band_of, False)
    return (increment, gradient)


MESH = pl.DeviceIdType.MESH
VMEM_BYTES = 64000 * 1024


def enter(n_wave, n_lev):
    me_w, me_l = lax.axis_index("wave"), lax.axis_index("lev")
    barrier = pltpu.get_barrier_semaphore()

    def greet(d, carry):
        peer = lax.rem(me_w + d, n_wave)
        pl.semaphore_signal(barrier, inc=1, device_id=(peer, me_l), device_id_type=MESH)
        return carry

    lax.fori_loop(1, n_wave, greet, 0)
    for d in range(1, n_lev):
        peer = lax.rem(me_l + d, n_lev)
        pl.semaphore_signal(barrier, inc=1, device_id=(me_w, peer), device_id_type=MESH)
    pl.semaphore_wait(barrier, n_wave + n_lev - 2)
    return me_w, me_l


def band_masks(wave, row0, rows, waves):
    total = wave + row0 + lax.broadcasted_iota(jnp.int32, (rows, LEVELS), 0)
    width = waves // COV_BANDS
    masks = []
    for b in range(COV_BANDS):
        hit = (total >= b * width) & (total < (b + 1) * width)
        masks.append(jnp.where(hit, 1.0, 0.0).astype(jnp.bfloat16))
    return masks


def banded_dot(x, masks, matrix):
    stacked = jnp.concatenate([x * mask for mask in masks], axis=1)
    return jnp.dot(stacked, matrix, preferred_element_type=jnp.float32).astype(jnp.bfloat16)


def forward_kernel(n_wave, n_lev, waves, waves_ref, x_ref, lt_ref, v_ref, out_ref,
                   spec, away, coef, wsend, x_send, x_recv, w_send, w_recv, own_sem):
    chunks, slots, rows, _ = x_ref.shape
    lats = lt_ref.shape[1] // n_wave
    per = v_ref.shape[0] // n_lev
    me_w, me_l = enter(n_wave, n_lev)
    row0 = me_l * rows

    def lev_copy(q, d):
        peer = lax.rem(me_l + d, n_lev)
        return pltpu.make_async_remote_copy(
            src_ref=away.at[q, d - 1], dst_ref=spec.at[q, me_l],
            send_sem=x_send.at[q, d - 1], recv_sem=x_recv.at[q, d - 1],
            device_id=(me_w, peer), device_id_type=MESH)

    def wave_copy(q, d):
        peer = lax.rem(me_w + d, n_wave)
        return pltpu.make_async_remote_copy(
            src_ref=wsend.at[q, peer], dst_ref=out_ref.at[q, me_w],
            send_sem=w_send.at[q, d - 1], recv_sem=w_recv.at[q, d - 1],
            device_id=(peer, me_l), device_id_type=MESH)

    def own_copy(q):
        return pltpu.make_async_copy(wsend.at[q, me_w], out_ref.at[q, me_w], own_sem.at[q])

    for q in range(chunks):
        def vertical_slot(s, carry):
            masks = band_masks(waves_ref[s], row0, rows, waves)
            for d in list(range(1, n_lev)) + [0]:
                half = lax.rem(me_l + d, n_lev)
                for i in range(per):
                    a = half * per + i
                    x = x_ref[q, s, :, pl.ds(pl.multiple_of(a * LEVELS, LEVELS), LEVELS)]
                    y = banded_dot(x, masks, v_ref[a])
                    if d == 0:
                        spec[q, me_l, s, :, i * LEVELS:(i + 1) * LEVELS] = y
                    else:
                        away[q, d - 1, s, :, i * LEVELS:(i + 1) * LEVELS] = y
            return carry

        lax.fori_loop(0, slots, vertical_slot, 0)
        for d in range(1, n_lev):
            lev_copy(q, d).start()

    for q in range(chunks):
        for d in range(1, n_lev):
            lev_copy(q, d).wait_recv()

        def legendre_slot(s, carry):
            field = jnp.concatenate([spec[q, l, s] for l in range(n_lev)], axis=0)
            coef[s] = jnp.dot(lt_ref[s], field, preferred_element_type=jnp.float32)
            return carry

        lax.fori_loop(0, slots, legendre_slot, 0)

        def turn(w, carry):
            for t in range(lats):
                wsend[q, w, t] = coef[:, w * lats + t, :].astype(jnp.bfloat16)
            return carry

        lax.fori_loop(0, n_wave, turn, 0)

        def send(d, carry):
            wave_copy(q, d).start()
            return carry

        lax.fori_loop(1, n_wave, send, 0)
        own_copy(q).start()

    for q in range(chunks):
        def finish(d, carry):
            wave_copy(q, d).wait()
            return carry

        lax.fori_loop(1, n_wave, finish, 0)
        own_copy(q).wait()
        for d in range(1, n_lev):
            lev_copy(q, d).wait_send()


def adjoint_kernel(n_wave, n_lev, waves, waves_ref, a_ref, l_ref, v_ref, out_ref,
                   land, fine, away, back, w_send, w_recv, x_send, x_recv):
    chunks, _, lats, slots, cols = a_ref.shape
    rows = out_ref.shape[2]
    per = v_ref.shape[0] // n_lev
    me_w, me_l = enter(n_wave, n_lev)
    row0 = me_l * rows

    def wave_copy(q, d):
        peer = lax.rem(me_w + d, n_wave)
        return pltpu.make_async_remote_copy(
            src_ref=a_ref.at[q, peer], dst_ref=land.at[q, me_w],
            send_sem=w_send.at[q, d - 1], recv_sem=w_recv.at[q, d - 1],
            device_id=(peer, me_l), device_id_type=MESH)

    def lev_copy(q, d):
        peer = lax.rem(me_l + d, n_lev)
        return pltpu.make_async_remote_copy(
            src_ref=away.at[q, d - 1], dst_ref=back.at[q, me_l],
            send_sem=x_send.at[q, d - 1], recv_sem=x_recv.at[q, d - 1],
            device_id=(me_w, peer), device_id_type=MESH)

    for q in range(chunks):
        def send(d, carry):
            wave_copy(q, d).start()
            return carry

        lax.fori_loop(1, n_wave, send, 0)
        land[q, me_w] = a_ref[q, me_w]

    for q in range(chunks):
        def arrive(d, carry):
            wave_copy(q, d).wait_recv()
            return carry

        lax.fori_loop(1, n_wave, arrive, 0)

        def widen(w, carry):
            base = pl.multiple_of(w * lats, lats)
            fine[pl.ds(base, lats)] = land[q, w].astype(jnp.float32)
            return carry

        lax.fori_loop(0, n_wave, widen, 0)

        def legendre_slot(s, carry):
            field = fine[:, s, :].astype(jnp.bfloat16)
            for d in range(n_lev):
                half = lax.rem(me_l + d, n_lev)
                table = l_ref[s, pl.ds(pl.multiple_of(half * rows, rows), rows), :]
                y = jnp.dot(table, field, preferred_element_type=jnp.float32).astype(jnp.bfloat16)
                if d == 0:
                    back[q, me_l, s] = y
                else:
                    away[q, d - 1, s] = y
            return carry

        lax.fori_loop(0, slots, legendre_slot, 0)
        for d in range(1, n_lev):
            lev_copy(q, d).start()

    for q in range(chunks):
        for d in range(1, n_lev):
            lev_copy(q, d).wait()

        def vertical_slot(s, carry):
            masks = band_masks(waves_ref[s], row0, rows, waves)
            for l in range(n_lev):
                for i in range(per):
                    a = l * per + i
                    x = back[q, l, s, :, i * LEVELS:(i + 1) * LEVELS]
                    out_ref[q, s, :, a * LEVELS:(a + 1) * LEVELS] = banded_dot(x, masks, v_ref[a])
            return carry

        lax.fori_loop(0, slots, vertical_slot, 0)

    for q in range(chunks):
        def drain(d, carry):
            wave_copy(q, d).wait_send()
            return carry

        lax.fori_loop(1, n_wave, drain, 0)


SIN_TERMS = [(-1.0) ** i * (2.0 * math.pi) ** (2 * i + 1) / math.factorial(2 * i + 1) for i in range(10)]
COS_TERMS = [(-1.0) ** i * (2.0 * math.pi) ** (2 * i) / math.factorial(2 * i) for i in range(10)]


def horner(terms, square):
    value = jnp.full_like(square, terms[-1])
    for term in terms[-2::-1]:
        value = value * square + term
    return value


def grid_kernel(waves_ref, points_ref, x_ref, scale_ref, weight_ref, inc_ref, adj_ref, table):
    members, _, cols, longs = inc_ref.shape
    waves = waves_ref.shape[0]
    points = points_ref[pl.program_id(0)]
    n = points.astype(jnp.float32)
    piece = 32
    inverse = 1.0 / jnp.full((1, longs), n, jnp.float32)
    lane = lax.broadcasted_iota(jnp.int32, (1, longs), 1)
    inside = jnp.where(lane < points, 1.0, 0.0) / math.sqrt(4.0 * waves)

    def build(i, carry):
        base = pl.multiple_of(i * piece, piece)
        wave = waves_ref[pl.ds(base, piece), :]
        product = wave * lane.astype(jnp.float32)
        turns = jnp.floor(product * inverse + 0.5)
        x = (product - turns * n) * inverse
        square = x * x
        gain = jnp.where(wave == 0.0, 1.0, 2.0) * inside
        table[pl.ds(base, piece), :] = (gain * horner(COS_TERMS, square)).astype(jnp.bfloat16)
        sine = (-gain) * (x * horner(SIN_TERMS, square))
        table[pl.ds(pl.multiple_of(waves + base, piece), piece), :] = sine.astype(jnp.bfloat16)
        return carry

    lax.fori_loop(0, waves // piece, build, 0)
    scale = scale_ref[0]
    for e in range(members):
        coeffs = jnp.concatenate([x_ref[2 * e + p, :, 0].reshape(waves, cols) for p in range(2)], axis=0)
        synthesis = lax.dot_general(coeffs, table[...], (((0,), (0,)), ((), ())),
                                    preferred_element_type=jnp.float32)
        increment = (synthesis * scale).astype(jnp.bfloat16)
        inc_ref[e, 0] = increment
        weighted = (increment.astype(jnp.float32) * weight_ref[0].astype(jnp.float32) * scale)
        adjoint = lax.dot_general(table[...], weighted.astype(jnp.bfloat16), (((1,), (1,)), ((), ())),
                                  preferred_element_type=jnp.float32).astype(jnp.bfloat16)
        for p in range(2):
            part = adjoint[p * waves:(p + 1) * waves]
            adj_ref[2 * e + p, :, 0] = part.reshape(adj_ref.shape[1], adj_ref.shape[3], cols)


def shards_kernels(n_wave, n_lev, control, wave_of_slot, legendre, vertical, points, lat_band, grid_scale, obs_weight):
    members, slots, rows = control.shape[:3]
    waves = wave_of_slot.shape[0]
    variables = vertical.shape[1]
    columns = control.shape[4]
    cols = columns // n_lev
    lats, _, longs = obs_weight.shape
    chunks = 2 * members
    bf16, f32 = jnp.bfloat16, jnp.float32
    own_waves = lax.dynamic_slice_in_dim(wave_of_slot, lax.axis_index("wave") * slots, slots)
    table = lax.all_gather(legendre, "lev", axis=1, tiled=True)
    x = control.transpose(0, 3, 1, 2, 4).reshape(chunks, slots, rows, columns)
    stack_f = vertical.transpose(1, 0, 3, 2).reshape(variables, COV_BANDS * LEVELS, LEVELS)
    stack_g = vertical.transpose(1, 0, 2, 3).reshape(variables, COV_BANDS * LEVELS, LEVELS)
    vmem = pl.BlockSpec(memory_space=pltpu.VMEM)
    smem = pl.BlockSpec(memory_space=pltpu.SMEM)
    dma = pltpu.SemaphoreType.DMA
    by_lat = pl.pallas_call(
        functools.partial(forward_kernel, n_wave, n_lev, waves),
        out_shape=jax.ShapeDtypeStruct((chunks, n_wave, lats, slots, cols), bf16),
        in_specs=[smem, vmem, vmem, vmem],
        out_specs=pl.BlockSpec(memory_space=pl.ANY),
        scratch_shapes=[
            pltpu.VMEM((chunks, n_lev, slots, rows, cols), bf16),
            pltpu.VMEM((chunks, n_lev - 1, slots, rows, cols), bf16),
            pltpu.VMEM((slots, n_wave * lats, cols), f32),
            pltpu.VMEM((chunks, n_wave, lats, slots, cols), bf16),
            dma((chunks, n_lev - 1)), dma((chunks, n_lev - 1)),
            dma((chunks, n_wave - 1)), dma((chunks, n_wave - 1)), dma((chunks,)),
        ],
        compiler_params=pltpu.CompilerParams(collective_id=0, has_side_effects=True, vmem_limit_bytes=VMEM_BYTES),
        name="forward",
    )(own_waves, x, table.transpose(0, 2, 1), stack_f)
    chooser = (
        lat_band[:, None] == jnp.arange(grid_scale.shape[0], dtype=jnp.int32)[None, :]
    ).astype(f32)
    lat_scale = jnp.dot(chooser, grid_scale, precision=lax.Precision.HIGHEST)
    field_spec = pl.BlockSpec((chunks, n_wave, 1, slots, cols), lambda t: (0, 0, t, 0, 0))
    increment, adjoint = pl.pallas_call(
        grid_kernel,
        grid=(lats,),
        out_shape=[
            jax.ShapeDtypeStruct((members, lats, cols, longs), bf16),
            jax.ShapeDtypeStruct((chunks, n_wave, lats, slots, cols), bf16),
        ],
        in_specs=[
            pl.BlockSpec((waves, 1), lambda t: (0, 0)),
            smem,
            field_spec,
            pl.BlockSpec((1, cols, 1), lambda t: (t, 0, 0)),
            pl.BlockSpec((1, cols, longs), lambda t: (t, 0, 0)),
        ],
        out_specs=[pl.BlockSpec((members, 1, cols, longs), lambda t: (0, t, 0, 0)), field_spec],
        scratch_shapes=[pltpu.VMEM((2 * waves, longs), bf16)],
        compiler_params=pltpu.CompilerParams(vmem_limit_bytes=VMEM_BYTES // 2),
        name="grid",
    )(wave_of_slot.astype(f32)[:, None], points, by_lat, lat_scale[:, :, None], obs_weight)
    gradient = pl.pallas_call(
        functools.partial(adjoint_kernel, n_wave, n_lev, waves),
        out_shape=jax.ShapeDtypeStruct((chunks, slots, rows, columns), bf16),
        in_specs=[smem, vmem, vmem, vmem],
        out_specs=vmem,
        scratch_shapes=[
            pltpu.VMEM((chunks, n_wave, lats, slots, cols), bf16),
            pltpu.VMEM((n_wave * lats, slots, cols), f32),
            pltpu.VMEM((chunks, n_lev - 1, slots, rows, cols), bf16),
            pltpu.VMEM((chunks, n_lev, slots, rows, cols), bf16),
            dma((chunks, n_wave - 1)), dma((chunks, n_wave - 1)),
            dma((chunks, n_lev - 1)), dma((chunks, n_lev - 1)),
        ],
        compiler_params=pltpu.CompilerParams(collective_id=1, has_side_effects=True, vmem_limit_bytes=VMEM_BYTES),
        name="adjoint",
    )(own_waves, adjoint, table, stack_g)
    gradient = gradient.reshape(members, 2, slots, rows, columns).transpose(0, 2, 3, 1, 4)
    return (increment, gradient)


def shards(n_wave, n_lev, *arrays):
    slots, rows, columns = arrays[0].shape[1], arrays[0].shape[2], arrays[0].shape[4]
    whole_tiles = slots % 16 == 0 and rows % 128 == 0 and columns % (n_lev * LEVELS) == 0
    if whole_tiles and n_lev > 1:
        return shards_kernels(n_wave, n_lev, *arrays)
    return shards_plain(*arrays)


def solution(mesh):
    in_specs = (
        P(None, "wave", "lev", None, None),
        P(),
        P("wave", "lev", None),
        P(),
        P("wave"),
        P("wave"),
        P(None, "lev"),
        P("wave", "lev", None),
    )
    out_specs = (P(None, "wave", "lev", None), P(None, "wave", "lev", None, None))
    body = functools.partial(shards, mesh.shape["wave"], mesh.shape["lev"])
    return jax.shard_map(body, mesh=mesh, in_specs=in_specs, out_specs=out_specs, check_vma=False)
```

```python
import functools
import math

import jax
import jax.numpy as jnp
from jax import lax
from jax.experimental import pallas as pl
from jax.experimental.pallas import tpu as pltpu
from jax.sharding import PartitionSpec as P

WAVES = 256
LONGITUDES = 512
LEVELS = 128
VARIABLES = 4
COV_BANDS = 4


def fourier_table(wave_ids, lat_points):
    lon_index = jnp.arange(LONGITUDES, dtype=jnp.int32)
    remainder = wave_ids[None, :, None] * lon_index[None, None, :] % lat_points[:, None, None]
    angles = (
        2.0
        * math.pi
        * remainder.astype(jnp.float32)
        / lat_points.astype(jnp.float32)[:, None, None]
    )
    factor = jnp.where(wave_ids == 0, 1.0, 2.0).astype(jnp.float32) / math.sqrt(4.0 * WAVES)
    inside = lon_index[None, None, :] < lat_points[:, None, None]
    cosine = jnp.where(inside, factor[None, :, None] * jnp.cos(angles), 0.0)
    sine = jnp.where(inside, -factor[None, :, None] * jnp.sin(angles), 0.0)
    return jnp.stack([cosine, sine], axis=2).astype(jnp.bfloat16)


def vertical_apply(field, vertical, live_rows, band_of, forward):
    members, slots, rows_dev = (field.shape[0], field.shape[1], field.shape[2])
    shaped = field.reshape(members, slots, rows_dev, 2, VARIABLES, LEVELS)
    form = "eskpam,alm->eskpal" if forward else "eskpal,alm->eskpam"
    summed = jnp.zeros(shaped.shape, jnp.float32)
    for index_band in range(COV_BANDS):
        partial_value = jnp.einsum(
            form, shaped, vertical[index_band], preferred_element_type=jnp.float32
        )
        chosen = live_rows & (band_of == index_band)
        summed = summed + jnp.where(chosen[None, :, :, None, None, None], partial_value, 0.0)
    return summed.reshape(field.shape).astype(jnp.bfloat16)


def to_bands(values):
    return lax.all_to_all(values, "wave", split_axis=2, concat_axis=1, tiled=True)


def shards_plain(control, wave_of_slot, legendre, vertical, points, lat_band, grid_scale, obs_weight):
    members, slots, rows_dev = (control.shape[0], control.shape[1], control.shape[2])
    slot_start = lax.axis_index("wave") * slots
    row_start = lax.axis_index("lev") * rows_dev
    own_waves = lax.dynamic_slice_in_dim(wave_of_slot, slot_start, slots)
    row_index = row_start + jnp.arange(rows_dev, dtype=jnp.int32)
    totals_n = own_waves[:, None] + row_index[None, :]
    live_rows = totals_n <= WAVES - 1
    band_of = jnp.minimum(totals_n * COV_BANDS // WAVES, COV_BANDS - 1)
    spectral = vertical_apply(control, vertical, live_rows, band_of, True)
    columns = lax.all_to_all(spectral, "lev", split_axis=4, concat_axis=2, tiled=True)
    col_dev = columns.shape[4]
    width = 2 * col_dev
    all_rows = columns.shape[2]
    columns = columns.reshape(members, slots, all_rows, width)
    coeffs = jnp.einsum(
        "skt,eskq->estq",
        lax.all_gather(legendre, "lev", axis=1, tiled=True),
        columns,
        preferred_element_type=jnp.float32,
    )
    coeffs = coeffs.astype(jnp.bfloat16)
    by_lat = to_bands(coeffs)
    wave_count = by_lat.shape[1]
    lat_dev = by_lat.shape[2]
    by_lat = by_lat.reshape(members, wave_count, lat_dev, 2, col_dev)
    fourier = fourier_table(wave_of_slot, points)
    synthesis = jnp.einsum("tspj,estpc->etcj", fourier, by_lat, preferred_element_type=jnp.float32)
    chooser = (
        lat_band[:, None] == jnp.arange(grid_scale.shape[0], dtype=jnp.int32)[None, :]
    ).astype(jnp.float32)
    lat_scale = jnp.dot(chooser, grid_scale, precision=lax.Precision.HIGHEST)
    increment = (synthesis * lat_scale[None, :, :, None]).astype(jnp.bfloat16)
    weighted = (
        increment.astype(jnp.float32) * obs_weight.astype(jnp.float32) * lat_scale[None, :, :, None]
    ).astype(jnp.bfloat16)
    adjoint_fourier = jnp.einsum(
        "tspj,etcj->etspc", fourier, weighted, preferred_element_type=jnp.float32
    )
    adjoint_fourier = adjoint_fourier.astype(jnp.bfloat16).reshape(
        members, lat_dev, wave_count, width
    )
    band_rows = to_bands(adjoint_fourier)
    adjoint_coeffs = jnp.einsum(
        "skt,etsq->eskq",
        lax.all_gather(legendre, "lev", axis=1, tiled=True),
        band_rows,
        preferred_element_type=jnp.float32,
    )
    adjoint_coeffs = adjoint_coeffs.astype(jnp.bfloat16).reshape(
        members, slots, all_rows, 2, col_dev
    )
    rows_back = lax.all_to_all(adjoint_coeffs, "lev", split_axis=2, concat_axis=4, tiled=True)
    gradient = vertical_apply(rows_back, vertical, live_rows, band_of, False)
    return (increment, gradient)


MESH = pl.DeviceIdType.MESH
VMEM_BYTES = 64000 * 1024


def enter(n_wave, n_lev):
    me_w, me_l = lax.axis_index("wave"), lax.axis_index("lev")
    barrier = pltpu.get_barrier_semaphore()

    def greet(d, carry):
        peer = lax.rem(me_w + d, n_wave)
        pl.semaphore_signal(barrier, inc=1, device_id=(peer, me_l), device_id_type=MESH)
        return carry

    lax.fori_loop(1, n_wave, greet, 0)
    for d in range(1, n_lev):
        peer = lax.rem(me_l + d, n_lev)
        pl.semaphore_signal(barrier, inc=1, device_id=(me_w, peer), device_id_type=MESH)
    pl.semaphore_wait(barrier, n_wave + n_lev - 2)
    return me_w, me_l


def band_masks(wave, row0, rows, waves):
    total = wave + row0 + lax.broadcasted_iota(jnp.int32, (rows, LEVELS), 0)
    width = waves // COV_BANDS
    masks = []
    for b in range(COV_BANDS):
        hit = (total >= b * width) & (total < (b + 1) * width)
        masks.append(jnp.where(hit, 1.0, 0.0).astype(jnp.bfloat16))
    return masks


def banded_dot(x, masks, matrix):
    stacked = jnp.concatenate([x * mask for mask in masks], axis=1)
    return jnp.dot(stacked, matrix, preferred_element_type=jnp.float32).astype(jnp.bfloat16)


def forward_kernel(n_wave, n_lev, waves, waves_ref, x_ref, l_ref, v_ref, out_ref, full_ref,
                   full, l_send, l_recv, full_sem, spec, away, coef, wsend, x_send, x_recv, w_send, w_recv, own_sem):
    chunks, slots, rows, _ = x_ref.shape
    lats = l_ref.shape[2] // n_wave
    per = v_ref.shape[0] // n_lev
    me_w, me_l = enter(n_wave, n_lev)
    row0 = me_l * rows

    def lev_copy(q, d):
        peer = lax.rem(me_l + d, n_lev)
        return pltpu.make_async_remote_copy(
            src_ref=away.at[q, d - 1], dst_ref=spec.at[q, me_l],
            send_sem=x_send.at[q, d - 1], recv_sem=x_recv.at[q, d - 1],
            device_id=(me_w, peer), device_id_type=MESH)

    def wave_copy(q, d):
        peer = lax.rem(me_w + d, n_wave)
        return pltpu.make_async_remote_copy(
            src_ref=wsend.at[q, peer], dst_ref=out_ref.at[q, me_w],
            send_sem=w_send.at[q, d - 1], recv_sem=w_recv.at[q, d - 1],
            device_id=(peer, me_l), device_id_type=MESH)

    def own_copy(q):
        return pltpu.make_async_copy(wsend.at[q, me_w], out_ref.at[q, me_w], own_sem.at[q])

    def table_copy(d):
        peer = lax.rem(me_l + d, n_lev)
        return pltpu.make_async_remote_copy(
            src_ref=l_ref, dst_ref=full.at[me_l],
            send_sem=l_send.at[d - 1], recv_sem=l_recv.at[d - 1],
            device_id=(me_w, peer), device_id_type=MESH)

    for d in range(1, n_lev):
        table_copy(d).start()
    full[me_l] = l_ref[...]
    keep = pltpu.make_async_copy(full, full_ref, full_sem)

    for q in range(chunks):
        def vertical_slot(s, carry):
            masks = band_masks(waves_ref[s], row0, rows, waves)
            for d in list(range(1, n_lev)) + [0]:
                half = lax.rem(me_l + d, n_lev)
                for i in range(per):
                    a = half * per + i
                    x = x_ref[q, s, :, pl.ds(pl.multiple_of(a * LEVELS, LEVELS), LEVELS)]
                    y = banded_dot(x, masks, v_ref[a])
                    if d == 0:
                        spec[q, me_l, s, :, i * LEVELS:(i + 1) * LEVELS] = y
                    else:
                        away[q, d - 1, s, :, i * LEVELS:(i + 1) * LEVELS] = y
            return carry

        lax.fori_loop(0, slots, vertical_slot, 0)
        for d in range(1, n_lev):
            lev_copy(q, d).start()

    for d in range(1, n_lev):
        table_copy(d).wait()
    keep.start()
    for q in range(chunks):
        for d in range(1, n_lev):
            lev_copy(q, d).wait_recv()

        def legendre_slot(s, carry):
            field = jnp.concatenate([spec[q, l, s] for l in range(n_lev)], axis=0)
            table = jnp.concatenate([full[l, s] for l in range(n_lev)], axis=0)
            coef[s] = lax.dot_general(table, field, (((0,), (0,)), ((), ())), preferred_element_type=jnp.float32)
            return carry

        lax.fori_loop(0, slots, legendre_slot, 0)

        def turn(w, carry):
            for t in range(lats):
                wsend[q, w, t] = coef[:, w * lats + t, :].astype(jnp.bfloat16)
            return carry

        lax.fori_loop(0, n_wave, turn, 0)

        def send(d, carry):
            wave_copy(q, d).start()
            return carry

        lax.fori_loop(1, n_wave, send, 0)
        own_copy(q).start()

    for q in range(chunks):
        def finish(d, carry):
            wave_copy(q, d).wait()
            return carry

        lax.fori_loop(1, n_wave, finish, 0)
        own_copy(q).wait()
        for d in range(1, n_lev):
            lev_copy(q, d).wait_send()
    keep.wait()


def adjoint_kernel(n_wave, n_lev, waves, waves_ref, a_ref, l_ref, v_ref, out_ref,
                   land, fine, away, back, w_send, w_recv, x_send, x_recv):
    chunks, _, lats, slots, cols = a_ref.shape
    rows = out_ref.shape[2]
    per = v_ref.shape[0] // n_lev
    me_w, me_l = enter(n_wave, n_lev)
    row0 = me_l * rows

    def wave_copy(q, d):
        peer = lax.rem(me_w + d, n_wave)
        return pltpu.make_async_remote_copy(
            src_ref=a_ref.at[q, peer], dst_ref=land.at[q, me_w],
            send_sem=w_send.at[q, d - 1], recv_sem=w_recv.at[q, d - 1],
            device_id=(peer, me_l), device_id_type=MESH)

    def lev_copy(q, d):
        peer = lax.rem(me_l + d, n_lev)
        return pltpu.make_async_remote_copy(
            src_ref=away.at[q, d - 1], dst_ref=back.at[q, me_l],
            send_sem=x_send.at[q, d - 1], recv_sem=x_recv.at[q, d - 1],
            device_id=(me_w, peer), device_id_type=MESH)

    for q in range(chunks):
        def send(d, carry):
            wave_copy(q, d).start()
            return carry

        lax.fori_loop(1, n_wave, send, 0)
        land[q, me_w] = a_ref[q, me_w]

    for q in range(chunks):
        def arrive(d, carry):
            wave_copy(q, d).wait_recv()
            return carry

        lax.fori_loop(1, n_wave, arrive, 0)

        def widen(w, carry):
            base = pl.multiple_of(w * lats, lats)
            fine[pl.ds(base, lats)] = land[q, w].astype(jnp.float32)
            return carry

        lax.fori_loop(0, n_wave, widen, 0)

        def legendre_slot(s, carry):
            field = fine[:, s, :].astype(jnp.bfloat16)
            for d in range(n_lev):
                half = lax.rem(me_l + d, n_lev)
                table = l_ref[half, s]
                y = jnp.dot(table, field, preferred_element_type=jnp.float32).astype(jnp.bfloat16)
                if d == 0:
                    back[q, me_l, s] = y
                else:
                    away[q, d - 1, s] = y
            return carry

        lax.fori_loop(0, slots, legendre_slot, 0)
        for d in range(1, n_lev):
            lev_copy(q, d).start()

    for q in range(chunks):
        for d in range(1, n_lev):
            lev_copy(q, d).wait()

        def vertical_slot(s, carry):
            masks = band_masks(waves_ref[s], row0, rows, waves)
            for l in range(n_lev):
                for i in range(per):
                    a = l * per + i
                    x = back[q, l, s, :, i * LEVELS:(i + 1) * LEVELS]
                    out_ref[q, s, :, a * LEVELS:(a + 1) * LEVELS] = banded_dot(x, masks, v_ref[a])
            return carry

        lax.fori_loop(0, slots, vertical_slot, 0)

    for q in range(chunks):
        def drain(d, carry):
            wave_copy(q, d).wait_send()
            return carry

        lax.fori_loop(1, n_wave, drain, 0)


SIN_TERMS = [(-1.0) ** i * (2.0 * math.pi) ** (2 * i + 1) / math.factorial(2 * i + 1) for i in range(10)]
COS_TERMS = [(-1.0) ** i * (2.0 * math.pi) ** (2 * i) / math.factorial(2 * i) for i in range(10)]


def horner(terms, square):
    value = jnp.full_like(square, terms[-1])
    for term in terms[-2::-1]:
        value = value * square + term
    return value


def grid_kernel(waves_ref, points_ref, x_ref, scale_ref, weight_ref, inc_ref, adj_ref, table):
    members, _, cols, longs = inc_ref.shape
    waves = waves_ref.shape[0]
    points = points_ref[pl.program_id(0)]
    n = points.astype(jnp.float32)
    piece = 32
    inverse = 1.0 / jnp.full((1, longs), n, jnp.float32)
    lane = lax.broadcasted_iota(jnp.int32, (1, longs), 1)
    inside = jnp.where(lane < points, 1.0, 0.0) / math.sqrt(4.0 * waves)

    def build(i, carry):
        base = pl.multiple_of(i * piece, piece)
        wave = waves_ref[pl.ds(base, piece), :]
        product = wave * lane.astype(jnp.float32)
        turns = jnp.floor(product * inverse + 0.5)
        x = (product - turns * n) * inverse
        square = x * x
        gain = jnp.where(wave == 0.0, 1.0, 2.0) * inside
        table[pl.ds(base, piece), :] = (gain * horner(COS_TERMS, square)).astype(jnp.bfloat16)
        sine = (-gain) * (x * horner(SIN_TERMS, square))
        table[pl.ds(pl.multiple_of(waves + base, piece), piece), :] = sine.astype(jnp.bfloat16)
        return carry

    lax.fori_loop(0, waves // piece, build, 0)
    scale = scale_ref[0]
    for e in range(members):
        coeffs = jnp.concatenate([x_ref[2 * e + p, :, 0].reshape(waves, cols) for p in range(2)], axis=0)
        synthesis = lax.dot_general(coeffs, table[...], (((0,), (0,)), ((), ())),
                                    preferred_element_type=jnp.float32)
        increment = (synthesis * scale).astype(jnp.bfloat16)
        inc_ref[e, 0] = increment
        weighted = (increment.astype(jnp.float32) * weight_ref[0].astype(jnp.float32) * scale)
        adjoint = lax.dot_general(table[...], weighted.astype(jnp.bfloat16), (((1,), (1,)), ((), ())),
                                  preferred_element_type=jnp.float32).astype(jnp.bfloat16)
        for p in range(2):
            part = adjoint[p * waves:(p + 1) * waves]
            adj_ref[2 * e + p, :, 0] = part.reshape(adj_ref.shape[1], adj_ref.shape[3], cols)


def shards_kernels(n_wave, n_lev, control, wave_of_slot, legendre, vertical, points, lat_band, grid_scale, obs_weight):
    members, slots, rows = control.shape[:3]
    waves = wave_of_slot.shape[0]
    variables = vertical.shape[1]
    columns = control.shape[4]
    cols = columns // n_lev
    lats, _, longs = obs_weight.shape
    chunks = 2 * members
    bf16, f32 = jnp.bfloat16, jnp.float32
    own_waves = lax.dynamic_slice_in_dim(wave_of_slot, lax.axis_index("wave") * slots, slots)
    x = control.transpose(0, 3, 1, 2, 4).reshape(chunks, slots, rows, columns)
    stack_f = vertical.transpose(1, 0, 3, 2).reshape(variables, COV_BANDS * LEVELS, LEVELS)
    stack_g = vertical.transpose(1, 0, 2, 3).reshape(variables, COV_BANDS * LEVELS, LEVELS)
    vmem = pl.BlockSpec(memory_space=pltpu.VMEM)
    smem = pl.BlockSpec(memory_space=pltpu.SMEM)
    dma = pltpu.SemaphoreType.DMA
    by_lat, table = pl.pallas_call(
        functools.partial(forward_kernel, n_wave, n_lev, waves),
        out_shape=[
            jax.ShapeDtypeStruct((chunks, n_wave, lats, slots, cols), bf16),
            jax.ShapeDtypeStruct((n_lev, *legendre.shape), bf16),
        ],
        in_specs=[smem, vmem, vmem, vmem],
        out_specs=[pl.BlockSpec(memory_space=pl.ANY)] * 2,
        scratch_shapes=[
            pltpu.VMEM((n_lev, *legendre.shape), bf16),
            dma((n_lev - 1,)), dma((n_lev - 1,)), dma,
            pltpu.VMEM((chunks, n_lev, slots, rows, cols), bf16),
            pltpu.VMEM((chunks, n_lev - 1, slots, rows, cols), bf16),
            pltpu.VMEM((slots, n_wave * lats, cols), f32),
            pltpu.VMEM((chunks, n_wave, lats, slots, cols), bf16),
            dma((chunks, n_lev - 1)), dma((chunks, n_lev - 1)),
            dma((chunks, n_wave - 1)), dma((chunks, n_wave - 1)), dma((chunks,)),
        ],
        compiler_params=pltpu.CompilerParams(collective_id=0, has_side_effects=True, vmem_limit_bytes=VMEM_BYTES),
        name="forward",
    )(own_waves, x, legendre, stack_f)
    chooser = (
        lat_band[:, None] == jnp.arange(grid_scale.shape[0], dtype=jnp.int32)[None, :]
    ).astype(f32)
    lat_scale = jnp.dot(chooser, grid_scale, precision=lax.Precision.HIGHEST)
    field_spec = pl.BlockSpec((chunks, n_wave, 1, slots, cols), lambda t: (0, 0, t, 0, 0))
    increment, adjoint = pl.pallas_call(
        grid_kernel,
        grid=(lats,),
        out_shape=[
            jax.ShapeDtypeStruct((members, lats, cols, longs), bf16),
            jax.ShapeDtypeStruct((chunks, n_wave, lats, slots, cols), bf16),
        ],
        in_specs=[
            pl.BlockSpec((waves, 1), lambda t: (0, 0)),
            smem,
            field_spec,
            pl.BlockSpec((1, cols, 1), lambda t: (t, 0, 0)),
            pl.BlockSpec((1, cols, longs), lambda t: (t, 0, 0)),
        ],
        out_specs=[pl.BlockSpec((members, 1, cols, longs), lambda t: (0, t, 0, 0)), field_spec],
        scratch_shapes=[pltpu.VMEM((2 * waves, longs), bf16)],
        compiler_params=pltpu.CompilerParams(vmem_limit_bytes=VMEM_BYTES // 2),
        name="grid",
    )(wave_of_slot.astype(f32)[:, None], points, by_lat, lat_scale[:, :, None], obs_weight)
    gradient = pl.pallas_call(
        functools.partial(adjoint_kernel, n_wave, n_lev, waves),
        out_shape=jax.ShapeDtypeStruct((chunks, slots, rows, columns), bf16),
        in_specs=[smem, vmem, vmem, vmem],
        out_specs=vmem,
        scratch_shapes=[
            pltpu.VMEM((chunks, n_wave, lats, slots, cols), bf16),
            pltpu.VMEM((n_wave * lats, slots, cols), f32),
            pltpu.VMEM((chunks, n_lev - 1, slots, rows, cols), bf16),
            pltpu.VMEM((chunks, n_lev, slots, rows, cols), bf16),
            dma((chunks, n_wave - 1)), dma((chunks, n_wave - 1)),
            dma((chunks, n_lev - 1)), dma((chunks, n_lev - 1)),
        ],
        compiler_params=pltpu.CompilerParams(collective_id=1, has_side_effects=True, vmem_limit_bytes=VMEM_BYTES),
        name="adjoint",
    )(own_waves, adjoint, table, stack_g)
    gradient = gradient.reshape(members, 2, slots, rows, columns).transpose(0, 2, 3, 1, 4)
    return (increment, gradient)


def shards(n_wave, n_lev, *arrays):
    slots, rows, columns = arrays[0].shape[1], arrays[0].shape[2], arrays[0].shape[4]
    whole_tiles = slots % 16 == 0 and rows % 128 == 0 and columns % (n_lev * LEVELS) == 0
    if whole_tiles and n_lev > 1:
        return shards_kernels(n_wave, n_lev, *arrays)
    return shards_plain(*arrays)


def solution(mesh):
    in_specs = (
        P(None, "wave", "lev", None, None),
        P(),
        P("wave", "lev", None),
        P(),
        P("wave"),
        P("wave"),
        P(None, "lev"),
        P("wave", "lev", None),
    )
    out_specs = (P(None, "wave", "lev", None), P(None, "wave", "lev", None, None))
    body = functools.partial(shards, mesh.shape["wave"], mesh.shape["lev"])
    return jax.shard_map(body, mesh=mesh, in_specs=in_specs, out_specs=out_specs, check_vma=False)
```
